512 devices in a mesh: space: 64 (over y, x, z_hi), tm: 8 (over z_lo, core).
Axes of the slice: x: 4, y: 8, z: 8 (z_hi: 2, z_lo: 4; z = z_hi * 4 + z_lo), core: 2. Of those that a mesh axis runs over, the one named last changes fastest.
Arguments:
- vectors: bfloat16 [8, 64, 2, 12, 8192], P('tm', None, None, None, 'space'), may hold values from -6 to 6
- dilution: int32 [64], replicated, may hold values from 0 to 23
- gamma_ids: int32 [16], replicated, may hold values from 1 to 15
Outputs:
- gram: float32 [8, 1024, 128], P(None, 'space')
- loops: float32 [8, 1024, 2], P(None, 'space')
The draws below stay inside these ranges and needn't reach their ends.
All inputs are finite; a program needn't handle non-finite values.
Results may differ from the reference program's by a relative error of at most 0.0003.
Values sent between devices are 32-bit elements; how exact they have to be, the bound alone decides.
A program may use at most 64 MiB of HBM per device.

```python
import math
from functools import partial
import jax
import jax.numpy as jnp
from jax import lax

NVEC = 64
NG = 16
TDIL = 2
NSITES = 8192
NT = 8


def touch_ends(result, rng, least, largest):
    shape = result.shape
    place = [jax.random.randint(jax.random.fold_in(rng, axis), (), 0, shape[axis]) for axis in range(len(shape))]
    result = result.at[tuple(place)].set(least)
    longest = shape.index(max(shape))
    place[longest] = (place[longest] + 1) % shape[longest]
    return result.at[tuple(place)].set(largest)


def level_of(own_key, extent, shards, smallest, largest):
    def one(dim, parts):
        steps = jax.random.uniform(jax.random.fold_in(jax.random.fold_in(own_key, 6), dim), (parts,), jnp.float32, smallest / len(shards), largest / len(shards))
        return jnp.repeat(jnp.exp(steps), extent[dim] // parts).reshape((-1,) + (1,) * (len(extent) - dim - 1))

    factor_of = one(*shards[0])
    for cut in shards[1:]:
        factor_of = factor_of * one(*cut)
    return factor_of


def noise(rng, dims, spread, bound, pieces=(), held_as=jnp.bfloat16):
    result = spread * jax.random.normal(rng, dims, jnp.float32)
    if pieces:
        result = result * level_of(rng, dims, pieces, -0.22, 0.18)
    return jnp.clip(result, -bound, bound).astype(held_as)


def setup_inputs(seed: int = 0) -> dict:
    arg_keys = jax.random.split(jax.random.key(seed), 4)
    return {
        "vectors": noise(arg_keys[0], (NT, NVEC, 2, 12, NSITES), 1.0, 6.0, ((0, 8), (4, 64))),
        "dilution": touch_ends(jax.random.randint(arg_keys[1], (NVEC,), 0, 12 * TDIL), jax.random.fold_in(arg_keys[1], 1), 0, (12 * TDIL) - 1).astype(jnp.int32),
        "gamma_ids": touch_ends(jax.random.randint(arg_keys[2], (NG,), 1, 16), jax.random.fold_in(arg_keys[2], 1), 1, 15).astype(jnp.int32),
    }


highest = lax.Precision.HIGHEST

def zero_square():
    return [[0, 0, 0, 0] for _ in range(4)]

def pair_product(left, right):
    real_out = zero_square()
    imag_out = zero_square()
    for row in range(4):
        for col in range(4):
            acc_real = 0
            acc_imag = 0
            for mid in range(4):
                acc_real += left[0][row][mid] * right[0][mid][col] - left[1][row][mid] * right[1][mid][col]
                acc_imag += left[0][row][mid] * right[1][mid][col] + left[1][row][mid] * right[0][mid][col]
            real_out[row][col] = acc_real
            imag_out[row][col] = acc_imag
    return (real_out, imag_out)

def dirac_tables():
    factors = [(zero_square(), [[0, 0, 0, 1], [0, 0, 1, 0], [0, -1, 0, 0], [-1, 0, 0, 0]]), ([[0, 0, 0, -1], [0, 0, 1, 0], [0, 1, 0, 0], [-1, 0, 0, 0]], zero_square()), (zero_square(), [[0, 0, 1, 0], [0, 0, 0, -1], [-1, 0, 0, 0], [0, 1, 0, 0]]), ([[0, 0, 1, 0], [0, 0, 0, 1], [1, 0, 0, 0], [0, 1, 0, 0]], zero_square())]
    reals = []
    imags = []
    for number in range(16):
        current = ([[1 if a == b else 0 for b in range(4)] for a in range(4)], zero_square())
        for position in range(4):
            if number >> position & 1:
                current = pair_product(current, factors[position])
        reals.append([value for line in current[0] for value in line])
        imags.append([value for line in current[1] for value in line])
    return (reals, imags)

def pick_gammas(gamma_ids):
    table_real, table_imag = dirac_tables()
    choose = (gamma_ids[:, None] == jnp.arange(16, dtype=jnp.int32)[None, :]).astype(jnp.float32)
    gamma_real = jnp.dot(choose, jnp.asarray(table_real, dtype=jnp.float32), precision=highest).reshape(-1, 4, 4)
    gamma_imag = jnp.dot(choose, jnp.asarray(table_imag, dtype=jnp.float32), precision=highest).reshape(-1, 4, 4)
    return (gamma_real, gamma_imag)

def reference(vectors, dilution, gamma_ids):
    times, count, halves, comps, sites = vectors.shape
    gamma_real, gamma_imag = pick_gammas(gamma_ids)
    gram_scale = 1.0 / math.sqrt(48.0 * sites)
    loop_scale = 1.0 / math.sqrt(1.0 * sites)
    spin_pick = ((dilution % 12 // 3)[:, None] == jnp.arange(4, dtype=jnp.int32)[None, :]).astype(jnp.float32)
    colour_pick = ((dilution % 3)[:, None] == jnp.arange(3, dtype=jnp.int32)[None, :]).astype(jnp.float32)
    time_class = dilution // 12
    ein = partial(jnp.einsum, precision=highest)

    def one_slice(inputs):
        block, slice_index = inputs
        field = block.astype(jnp.float32).reshape(count, 2, 4, 3, sites)
        real_part = field[:, 0]
        imag_part = field[:, 1]
        pair_real = ein('iack,jbck->iajb', real_part, real_part) + ein('iack,jbck->iajb', imag_part, imag_part)
        pair_imag = ein('iack,jbck->iajb', real_part, imag_part) - ein('iack,jbck->iajb', imag_part, real_part)
        gram_real = ein('gab,iajb->gij', gamma_real, pair_real) - ein('gab,iajb->gij', gamma_imag, pair_imag)
        gram_imag = ein('gab,iajb->gij', gamma_real, pair_imag) + ein('gab,iajb->gij', gamma_imag, pair_real)
        gram = jnp.concatenate([gram_real, gram_imag], axis=2).reshape(-1, 2 * count) * gram_scale
        site_sums = lax.optimization_barrier(jnp.sum(field, axis=-1))
        picked = ein('ipac,ic->ipa', site_sums, colour_pick)
        rows_real = ein('gba,ib->gia', gamma_real, spin_pick)
        rows_imag = ein('gba,ib->gia', gamma_imag, spin_pick)
        loop_real = ein('gia,ia->gi', rows_real, picked[:, 0]) - ein('gia,ia->gi', rows_imag, picked[:, 1])
        loop_imag = ein('gia,ia->gi', rows_real, picked[:, 1]) + ein('gia,ia->gi', rows_imag, picked[:, 0])
        live = (time_class == slice_index % TDIL).astype(jnp.float32)[None, :]
        loops = jnp.stack([loop_real * live, loop_imag * live], axis=-1).reshape(-1, 2) * loop_scale
        return (gram, loops)
    gram, loops = lax.map(one_slice, (vectors, jnp.arange(times, dtype=jnp.int32)))
    return (gram, loops)
```

```python
from functools import partial
import math

import jax
import jax.numpy as jnp
import numpy as np
from jax import lax
from jax.experimental import pallas as pl
from jax.experimental.pallas import tpu as pltpu
from jax.sharding import PartitionSpec as P

NV = 64
NG = 16
NY = 8
NX = 4
NZH = 2
NTM = 8
ORDER = (4, 3, 5, 2, 6, 1, 7, 0)
MESH = pl.DeviceIdType.MESH


def dirac_table():
    i = 1j
    gammas = [
        np.array([[0, 0, 0, i], [0, 0, i, 0], [0, -i, 0, 0], [-i, 0, 0, 0]]),
        np.array([[0, 0, 0, -1], [0, 0, 1, 0], [0, 1, 0, 0], [-1, 0, 0, 0]], complex),
        np.array([[0, 0, i, 0], [0, 0, 0, -i], [-i, 0, 0, 0], [0, i, 0, 0]]),
        np.array([[0, 0, 1, 0], [0, 0, 0, 1], [1, 0, 0, 0], [0, 1, 0, 0]], complex),
    ]
    rows = []
    for number in range(16):
        product = np.eye(4, dtype=complex)
        for bit in range(4):
            if number >> bit & 1:
                product = product @ gammas[bit]
        m = int(np.flatnonzero(product[0])[0])
        phase = product[0, m]
        found = None
        for w in range(4):
            signs = [(-1) ** bin(w & a).count("1") for a in range(4)]
            trial = np.zeros((4, 4), complex)
            for a in range(4):
                trial[a, a ^ m] = phase * signs[a]
            if np.array_equal(trial, product):
                found = w
        eps = (-1) ** bin(found & m).count("1")
        rows.append((m, found, int(phase.real), int(phase.imag), eps))
    return rows


TABLE = dirac_table()


def pick(number, values):
    out = jnp.float32(values[0])
    for k in range(1, 16):
        if values[k] != values[0]:
            out = jnp.where(number == k, jnp.float32(values[k]), out)
    return out


def kernel(
    gram_scale,
    loop_scale,
    gid_ref,
    dil_ref,
    v_hbm,
    gram_ref,
    loop_ref,
    vb,
    vf,
    lhs,
    dmat,
    tabs,
    ltab,
    xbuf,
    xrecv,
    ysend,
    yrecv,
    yrecv2,
    zsend,
    zrecv,
    xl,
    xlrecv,
    yl,
    ylrecv,
    zl,
    zlrecv,
    in_sem,
    x_send,
    x_recv,
    y_send,
    y_recv,
    y2_send,
    y2_recv,
    z_send,
    z_recv,
    xl_send,
    xl_recv,
    yl_send,
    yl_recv,
    zl_send,
    zl_recv,
):
    space = lax.axis_index("space")
    tm = lax.axis_index("tm")
    y = space // 8
    x = (space // 2) % 4
    zh = space % 2
    p = x % 2
    xp = x + 1 - 2 * p

    load = pltpu.make_async_copy(v_hbm, vb, in_sem)
    load.start()

    def at(y_, x_, zh_, tm_):
        return (y_ * 8 + x_ * 2 + zh_, tm_)

    barrier = pltpu.get_barrier_semaphore()
    partners = []
    for k in range(1, NX):
        partners.append(at(y, (x + k) % NX, zh, tm))
    for k in range(1, NY):
        partners.append(at((y + k) % NY, x, zh, tm))
        partners.append(at((y + k) % NY, xp, zh, tm))
    for kz in range(NZH):
        for kt in range(NTM):
            if kz or kt:
                partners.append(at(y, x, (zh + kz) % NZH, (tm + kt) % NTM))
    for who in partners:
        pl.semaphore_signal(barrier, inc=1, device_id=who, device_id_type=MESH)

    lane = lax.broadcasted_iota(jnp.int32, (8, 128), 1)
    group = lane // 32
    low = lane < 64
    low1 = lax.broadcasted_iota(jnp.int32, (1, 128), 1) < 64

    load.wait()
    vf[...] = vb[...].astype(jnp.float32)
    for a in range(4):
        for c in range(3):
            start = 2 * (3 * a + c)
            re = vf[pl.ds(start, NV, stride=24), :].astype(jnp.bfloat16)
            im = vf[pl.ds(start + 1, NV, stride=24), :].astype(jnp.bfloat16)
            first = slice(a * 64, a * 64 + 64)
            second = slice(256 + a * 64, 256 + a * 64 + 64)
            kr = slice(c * 128, c * 128 + 128)
            ki = slice((3 + c) * 128, (3 + c) * 128 + 128)
            lhs[first, kr] = re
            lhs[first, ki] = im
            lhs[second, kr] = -im
            lhs[second, ki] = re
    block = lax.broadcasted_iota(jnp.int32, (16, 768), 1) // 128
    row = lax.broadcasted_iota(jnp.int32, (16, 768), 0)
    lhs[512:528, :] = jnp.where(block == row, 1.0, 0.0).astype(jnp.bfloat16)
    prod = lax.dot_general(
        lhs[...], lhs[0:256, :], (((1,), (1,)), ((), ())), preferred_element_type=jnp.float32
    )
    dmat[...] = prod[0:256] + prod[256:512]
    sums = prod[512:528]

    for m in range(4):
        for pp in range(2):
            for qq in range(2):
                parts = []
                for a in range(4):
                    b = a ^ m
                    grp = 2 * (b & 1) + qq
                    tile = None
                    for ib in range(4):
                        r0 = a * 64 + (4 * pp + ib) * 8
                        c0 = (b // 2) * 128
                        piece = dmat[r0 : r0 + 8, c0 : c0 + 128]
                        shift = (32 * (ib - grp)) % 128
                        if shift:
                            piece = pltpu.roll(piece, shift, 1)
                        tile = piece if tile is None else jnp.where(group == ib, piece, tile)
                    parts.append(tile)
                s01, d01 = parts[0] + parts[1], parts[0] - parts[1]
                s23, d23 = parts[2] + parts[3], parts[2] - parts[3]
                combos = (s01 + s23, d01 + d23, s01 - s23, d01 - d23)
                slot = 0 if pp == qq else 1
                for number in range(16):
                    if TABLE[number][0] == m:
                        tabs[number, pp, 8 * slot : 8 * slot + 8, :] = combos[TABLE[number][1]]

    dil = dil_ref[...]
    dil = jnp.concatenate([dil, dil], axis=1)
    klass = (dil >= 12).astype(jnp.int32)
    d12 = dil - 12 * klass
    spin = (
        (d12 >= 3).astype(jnp.int32) + (d12 >= 6).astype(jnp.int32) + (d12 >= 9).astype(jnp.int32)
    )
    colour = d12 - 3 * spin
    live = jnp.where(klass == tm % 2, jnp.float32(loop_scale), jnp.float32(0.0))

    def coloured(h, half):
        out = jnp.zeros((1, 128), jnp.float32)
        for c in range(3):
            line = sums[3 * h + c : 3 * h + c + 1, half * 128 : half * 128 + 128]
            out = out + jnp.where(colour == c, line, 0.0)
        return out

    lines = []
    for half in range(2):
        re, im = coloured(0, half), coloured(1, half)
        lines.append(jnp.where(low1, re, pltpu.roll(im, 64, 1)) * live)
        lines.append(jnp.where(low1, pltpu.roll(re, 64, 1), im) * live)
    picked = []
    for m in range(4):
        out = jnp.zeros((1, 128), jnp.float32)
        for r in range(4):
            out = out + jnp.where(spin == (r ^ m), lines[r], 0.0)
        picked.append(out)
    for number in range(16):
        m, w = TABLE[number][0], TABLE[number][1]
        odd = jnp.zeros((1, 128), jnp.int32)
        for bit in range(2):
            if w >> bit & 1:
                odd = odd + (spin // (1 << bit)) % 2
        ltab[number] = jnp.where(odd == 1, -picked[m], picked[m])

    for g in range(NG):
        number = gid_ref[g]
        xbuf[2 * (g % 2), g // 2] = tabs[number, 0]
        xbuf[2 * (g % 2) + 1, g // 2] = tabs[number, 1]
        xl[g % 2, g // 2] = ltab[number]

    pl.semaphore_wait(barrier, len(partners))

    for j in range(NY):
        to_y = (y + ORDER[j]) % NY
        for k in range(1, NX):
            to_x = (x + k) % NX
            pltpu.make_async_remote_copy(
                src_ref=xbuf.at[to_x, to_y],
                dst_ref=xrecv.at[j, k - 1],
                send_sem=x_send,
                recv_sem=x_recv.at[j],
                device_id=at(y, to_x, zh, tm),
                device_id_type=MESH,
            ).start()
        if j == 0:
            for k in range(1, NX):
                to_x = (x + k) % NX
                pltpu.make_async_remote_copy(
                    src_ref=xl.at[to_x // 2],
                    dst_ref=xlrecv.at[k - 1],
                    send_sem=xl_send,
                    recv_sem=xl_recv,
                    device_id=at(y, to_x, zh, tm),
                    device_id_type=MESH,
                ).start()

    for j in range(NY):
        to_y = (y + ORDER[j]) % NY
        pltpu.make_async_copy(xrecv.at[j], xrecv.at[j], x_recv.at[j]).wait()
        ysend[j] = (xbuf[x, to_y] + xrecv[j, 0]) + (xrecv[j, 1] + xrecv[j, 2])
        pltpu.make_async_remote_copy(
            src_ref=ysend.at[j, pl.ds(8, 8)],
            dst_ref=yrecv2.at[j],
            send_sem=y2_send,
            recv_sem=y2_recv,
            device_id=at(to_y, xp, zh, tm),
            device_id_type=MESH,
        ).start()
        if j < NY - 1:
            pltpu.make_async_remote_copy(
                src_ref=ysend.at[j],
                dst_ref=yrecv.at[j],
                send_sem=y_send,
                recv_sem=y_recv,
                device_id=at(to_y, x, zh, tm),
                device_id_type=MESH,
            ).start()
        if j == 0:
            pltpu.make_async_copy(xlrecv, xlrecv, xl_recv).wait()
            yl[...] = (xl[x // 2] + xlrecv[0]) + (xlrecv[1] + xlrecv[2])
            for i in range(NY - 1):
                line_y = (y + ORDER[i]) % NY
                pltpu.make_async_remote_copy(
                    src_ref=yl.at[line_y],
                    dst_ref=ylrecv.at[i],
                    send_sem=yl_send,
                    recv_sem=yl_recv,
                    device_id=at(line_y, x, zh, tm),
                    device_id_type=MESH,
                ).start()

    pltpu.make_async_copy(ylrecv, ylrecv, yl_recv).wait()
    total = yl[y]
    for i in range(NY - 1):
        total = total + ylrecv[i]
    zl[...] = total
    zlrecv[zh * NTM + tm] = total
    for kz in range(NZH):
        for kt in range(NTM):
            if kz or kt:
                pltpu.make_async_remote_copy(
                    src_ref=zl,
                    dst_ref=zlrecv.at[zh * NTM + tm],
                    send_sem=zl_send,
                    recv_sem=zl_recv,
                    device_id=at(y, x, (zh + kz) % NZH, (tm + kt) % NTM),
                    device_id_type=MESH,
                ).start()

    pltpu.make_async_copy(yrecv, yrecv, y_recv).wait()
    pltpu.make_async_copy(yrecv2, yrecv2, y2_recv).wait()
    own = ysend[NY - 1]
    for j in range(NY - 1):
        own = own + yrecv[j]
    other = yrecv2[0]
    for j in range(1, NY):
        other = other + yrecv2[j]
    diag, off = own[0:8], own[8:16]
    first = p == 0
    left, right = jnp.where(first, diag, off), jnp.where(first, off, diag)
    upper, lower = jnp.where(first, diag, other), jnp.where(first, other, diag)

    def turned(tile, shift):
        shift = shift % 128
        return pltpu.roll(tile, shift, 1) if shift else tile

    columns = [turned(t, -32 * ib) for t in (upper, lower) for ib in range(4)]
    columns = jnp.concatenate(columns + columns, axis=0)
    flipped = columns.T
    for ib in range(4):
        r0 = 8 * ib
        rows = jnp.where(lane < 32, turned(left, -32 * ib), turned(right, 32 - 32 * ib))
        rows = jnp.where(low, rows, flipped[r0 : r0 + 8])
        zsend[ib // 2, 8 * (ib % 2) : 8 * (ib % 2) + 8, :] = rows
    zrecv[zh * NTM + tm] = zsend[zh]
    for kz in range(NZH):
        for kt in range(NTM):
            if kz or kt:
                to_z = (zh + kz) % NZH
                pltpu.make_async_remote_copy(
                    src_ref=zsend.at[to_z],
                    dst_ref=zrecv.at[zh * NTM + tm],
                    send_sem=z_send,
                    recv_sem=z_recv,
                    device_id=at(y, x, to_z, (tm + kt) % NTM),
                    device_id_type=MESH,
                ).start()

    number = gid_ref[2 * y + x // 2]
    half = 0.5 * gram_scale
    re_t = pick(number, [half * (t[2] - t[3]) for t in TABLE])
    re_f = pick(number, [half * t[4] * (t[2] + t[3]) for t in TABLE])
    im_t = pick(number, [half * (t[2] + t[3]) for t in TABLE])
    im_f = pick(number, [half * t[4] * (t[3] - t[2]) for t in TABLE])
    phase_re = pick(number, [float(t[2]) for t in TABLE])
    phase_im = pick(number, [float(t[3]) for t in TABLE])
    straight = jnp.where(low1, re_t, im_f)
    crossed = jnp.where(low1, re_f, im_t)
    turn = jnp.where(low1, -phase_im, phase_im)

    pltpu.make_async_copy(zlrecv.at[pl.ds(0, 15)], zlrecv.at[pl.ds(0, 15)], zl_recv).wait()
    value = (zlrecv[0:NTM] + zlrecv[NTM : 2 * NTM]).reshape(NTM, 128)
    value = phase_re * value + turn * pltpu.roll(value, 64, 1)
    value = pltpu.roll(value, (128 - 16 * (2 * p + zh)) % 128, 1)
    loop_ref[:, 0, :] = value[:, 0:16]
    loop_ref[:, 1, :] = value[:, 64:80]

    pltpu.make_async_copy(zrecv.at[pl.ds(0, 15)], zrecv.at[pl.ds(0, 15)], z_recv).wait()
    for t in range(NTM):
        value = zrecv[t] + zrecv[NTM + t]
        gram_ref[t] = straight * value + crossed * pltpu.roll(value, 64, 1)

    pltpu.make_async_copy(xbuf.at[pl.ds(0, 3)], xbuf.at[pl.ds(0, 3)], x_send).wait()
    pltpu.make_async_copy(xlrecv, xlrecv, xl_send).wait()
    pltpu.make_async_copy(yrecv, yrecv, y_send).wait()
    pltpu.make_async_copy(yrecv2, yrecv2, y2_send).wait()
    pltpu.make_async_copy(ylrecv, ylrecv, yl_send).wait()
    pltpu.make_async_copy(zrecv.at[pl.ds(0, 15)], zrecv.at[pl.ds(0, 15)], z_send).wait()
    pltpu.make_async_copy(zlrecv.at[pl.ds(0, 15)], zlrecv.at[pl.ds(0, 15)], zl_send).wait()


def shards(vectors, dilution, gamma_ids):
    slices, count, halves, comps, sites = vectors.shape
    total_sites = sites * lax.axis_size("space")
    gram_scale = 1.0 / math.sqrt(48.0 * total_sites)
    loop_scale = 1.0 / math.sqrt(1.0 * total_sites)
    flat = vectors.transpose(0, 1, 3, 2, 4).reshape(count * comps * halves, sites)
    f32, bf16 = jnp.float32, jnp.bfloat16
    dma = pltpu.SemaphoreType.DMA
    vmem = pltpu.VMEM
    gram, loops = pl.pallas_call(
        partial(kernel, gram_scale, loop_scale),
        out_shape=(
            jax.ShapeDtypeStruct((NTM, 16, 128), f32),
            jax.ShapeDtypeStruct((NTM, 2, 16), f32),
        ),
        in_specs=[
            pl.BlockSpec(memory_space=pltpu.SMEM),
            pl.BlockSpec(memory_space=pltpu.VMEM),
            pl.BlockSpec(memory_space=pl.ANY),
        ],
        out_specs=(
            pl.BlockSpec(memory_space=pltpu.VMEM),
            pl.BlockSpec(memory_space=pltpu.VMEM),
        ),
        scratch_shapes=[
            vmem((1536, 128), bf16),
            vmem((1536, 128), f32),
            vmem((528, 768), bf16),
            vmem((256, 256), f32),
            vmem((16, 2, 16, 128), f32),
            vmem((16, 1, 128), f32),
            vmem((NX, NY, 16, 128), f32),
            vmem((NY, NX - 1, 16, 128), f32),
            vmem((NY, 16, 128), f32),
            vmem((NY - 1, 16, 128), f32),
            vmem((NY, 8, 128), f32),
            vmem((NZH, 16, 128), f32),
            vmem((NZH * NTM, 16, 128), f32),
            vmem((2, NY, 1, 128), f32),
            vmem((NX - 1, NY, 1, 128), f32),
            vmem((NY, 1, 128), f32),
            vmem((NY - 1, 1, 128), f32),
            vmem((1, 128), f32),
            vmem((NZH * NTM, 1, 128), f32),
            dma,
            dma,
            dma((NY,)),
        ]
        + [dma] * 12,
        compiler_params=pltpu.CompilerParams(collective_id=0, has_side_effects=True),
        name="gram_loops",
    )(gamma_ids, dilution.reshape(1, count), flat)
    return gram, loops.transpose(0, 2, 1)


def solution(mesh):
    placed = (P("tm", None, None, None, "space"), P(), P())
    return jax.shard_map(
        shards,
        mesh=mesh,
        in_specs=placed,
        out_specs=(P(None, "space", None), P(None, "space", None)),
        check_vma=False,
    )
```

```python
from functools import partial
import math

import jax
import jax.numpy as jnp
import numpy as np
from jax import lax
from jax.experimental import pallas as pl
from jax.experimental.pallas import tpu as pltpu
from jax.sharding import PartitionSpec as P

NV = 64
NG = 16
NY = 8
NX = 4
NZH = 2
NTM = 8
ORDER = (4, 3, 5, 2, 6, 1, 7, 0)
MESH = pl.DeviceIdType.MESH


def dirac_table():
    i = 1j
    gammas = [
        np.array([[0, 0, 0, i], [0, 0, i, 0], [0, -i, 0, 0], [-i, 0, 0, 0]]),
        np.array([[0, 0, 0, -1], [0, 0, 1, 0], [0, 1, 0, 0], [-1, 0, 0, 0]], complex),
        np.array([[0, 0, i, 0], [0, 0, 0, -i], [-i, 0, 0, 0], [0, i, 0, 0]]),
        np.array([[0, 0, 1, 0], [0, 0, 0, 1], [1, 0, 0, 0], [0, 1, 0, 0]], complex),
    ]
    rows = []
    for number in range(16):
        product = np.eye(4, dtype=complex)
        for bit in range(4):
            if number >> bit & 1:
                product = product @ gammas[bit]
        m = int(np.flatnonzero(product[0])[0])
        phase = product[0, m]
        found = None
        for w in range(4):
            signs = [(-1) ** bin(w & a).count("1") for a in range(4)]
            trial = np.zeros((4, 4), complex)
            for a in range(4):
                trial[a, a ^ m] = phase * signs[a]
            if np.array_equal(trial, product):
                found = w
        eps = (-1) ** bin(found & m).count("1")
        rows.append((m, found, int(phase.real), int(phase.imag), eps))
    return rows


TABLE = dirac_table()


def pick(number, values):
    out = jnp.float32(values[0])
    for k in range(1, 16):
        if values[k] != values[0]:
            out = jnp.where(number == k, jnp.float32(values[k]), out)
    return out


def kernel(
    gram_scale,
    loop_scale,
    gid_hbm,
    dil_hbm,
    v_hbm,
    gram_ref,
    loop_ref,
    gid_ref,
    dil_ref,
    vb,
    vf,
    lhs,
    dmat,
    tabs,
    ltab,
    xbuf,
    xrecv,
    ysend,
    yrecv,
    yrecv2,
    zsend,
    zrecv,
    xl,
    xlrecv,
    yl,
    ylrecv,
    zl,
    zlrecv,
    in_sem,
    gid_sem,
    dil_sem,
    x_send,
    x_recv,
    y_send,
    y_recv,
    y2_send,
    y2_recv,
    z_send,
    z_recv,
    xl_send,
    xl_recv,
    yl_send,
    yl_recv,
    zl_send,
    zl_recv,
):
    space = lax.axis_index("space")
    tm = lax.axis_index("tm")
    y = space // 8
    x = (space // 2) % 4
    zh = space % 2
    p = x % 2
    xp = x + 1 - 2 * p

    load = pltpu.make_async_copy(v_hbm, vb, in_sem)
    load.start()
    load_gid = pltpu.make_async_copy(gid_hbm, gid_ref, gid_sem)
    load_gid.start()
    load_dil = pltpu.make_async_copy(dil_hbm, dil_ref, dil_sem)
    load_dil.start()

    def at(y_, x_, zh_, tm_):
        return (y_ * 8 + x_ * 2 + zh_, tm_)

    barrier = pltpu.get_barrier_semaphore()
    partners = []
    for k in range(1, NX):
        partners.append(at(y, (x + k) % NX, zh, tm))
    for k in range(1, NY):
        partners.append(at((y + k) % NY, x, zh, tm))
        partners.append(at((y + k) % NY, xp, zh, tm))
    for kz in range(NZH):
        for kt in range(NTM):
            if kz or kt:
                partners.append(at(y, x, (zh + kz) % NZH, (tm + kt) % NTM))
    for who in partners:
        pl.semaphore_signal(barrier, inc=1, device_id=who, device_id_type=MESH)

    lane = lax.broadcasted_iota(jnp.int32, (8, 128), 1)
    group = lane // 32
    low = lane < 64
    low1 = lax.broadcasted_iota(jnp.int32, (1, 128), 1) < 64

    load.wait()
    vf[...] = vb[...].astype(jnp.float32)
    for a in range(4):
        for c in range(3):
            start = 2 * (3 * a + c)
            re = vf[pl.ds(start, NV, stride=24), :].astype(jnp.bfloat16)
            im = vf[pl.ds(start + 1, NV, stride=24), :].astype(jnp.bfloat16)
            first = slice(a * 64, a * 64 + 64)
            second = slice(256 + a * 64, 256 + a * 64 + 64)
            kr = slice(c * 128, c * 128 + 128)
            ki = slice((3 + c) * 128, (3 + c) * 128 + 128)
            lhs[first, kr] = re
            lhs[first, ki] = im
            lhs[second, kr] = -im
            lhs[second, ki] = re
    block = lax.broadcasted_iota(jnp.int32, (16, 768), 1) // 128
    row = lax.broadcasted_iota(jnp.int32, (16, 768), 0)
    lhs[512:528, :] = jnp.where(block == row, 1.0, 0.0).astype(jnp.bfloat16)
    prod = lax.dot_general(
        lhs[...], lhs[0:256, :], (((1,), (1,)), ((), ())), preferred_element_type=jnp.float32
    )
    dmat[...] = prod[0:256] + prod[256:512]
    sums = prod[512:528]

    for m in range(4):
        for pp in range(2):
            for qq in range(2):
                parts = []
                for a in range(4):
                    b = a ^ m
                    grp = 2 * (b & 1) + qq
                    tile = None
                    for ib in range(4):
                        r0 = a * 64 + (4 * pp + ib) * 8
                        c0 = (b // 2) * 128
                        piece = dmat[r0 : r0 + 8, c0 : c0 + 128]
                        shift = (32 * (ib - grp)) % 128
                        if shift:
                            piece = pltpu.roll(piece, shift, 1)
                        tile = piece if tile is None else jnp.where(group == ib, piece, tile)
                    parts.append(tile)
                s01, d01 = parts[0] + parts[1], parts[0] - parts[1]
                s23, d23 = parts[2] + parts[3], parts[2] - parts[3]
                combos = (s01 + s23, d01 + d23, s01 - s23, d01 - d23)
                slot = 0 if pp == qq else 1
                for number in range(16):
                    if TABLE[number][0] == m:
                        tabs[number, pp, 8 * slot : 8 * slot + 8, :] = combos[TABLE[number][1]]

    load_dil.wait()
    dil = dil_ref[...]
    dil = jnp.concatenate([dil, dil], axis=1)
    klass = (dil >= 12).astype(jnp.int32)
    d12 = dil - 12 * klass
    spin = (
        (d12 >= 3).astype(jnp.int32) + (d12 >= 6).astype(jnp.int32) + (d12 >= 9).astype(jnp.int32)
    )
    colour = d12 - 3 * spin
    live = jnp.where(klass == tm % 2, jnp.float32(loop_scale), jnp.float32(0.0))

    def coloured(h, half):
        out = jnp.zeros((1, 128), jnp.float32)
        for c in range(3):
            line = sums[3 * h + c : 3 * h + c + 1, half * 128 : half * 128 + 128]
            out = out + jnp.where(colour == c, line, 0.0)
        return out

    lines = []
    for half in range(2):
        re, im = coloured(0, half), coloured(1, half)
        lines.append(jnp.where(low1, re, pltpu.roll(im, 64, 1)) * live)
        lines.append(jnp.where(low1, pltpu.roll(re, 64, 1), im) * live)
    picked = []
    for m in range(4):
        out = jnp.zeros((1, 128), jnp.float32)
        for r in range(4):
            out = out + jnp.where(spin == (r ^ m), lines[r], 0.0)
        picked.append(out)
    for number in range(16):
        m, w = TABLE[number][0], TABLE[number][1]
        odd = jnp.zeros((1, 128), jnp.int32)
        for bit in range(2):
            if w >> bit & 1:
                odd = odd + (spin // (1 << bit)) % 2
        ltab[number] = jnp.where(odd == 1, -picked[m], picked[m])

    load_gid.wait()
    for g in range(NG):
        number = gid_ref[g]
        xbuf[2 * (g % 2), g // 2] = tabs[number, 0]
        xbuf[2 * (g % 2) + 1, g // 2] = tabs[number, 1]
        xl[g % 2, g // 2] = ltab[number]

    pl.semaphore_wait(barrier, len(partners))

    for j in range(NY):
        to_y = (y + ORDER[j]) % NY
        for k in range(1, NX):
            to_x = (x + k) % NX
            pltpu.make_async_remote_copy(
                src_ref=xbuf.at[to_x, to_y],
                dst_ref=xrecv.at[j, k - 1],
                send_sem=x_send,
                recv_sem=x_recv.at[j],
                device_id=at(y, to_x, zh, tm),
                device_id_type=MESH,
            ).start()
        if j == 0:
            for k in range(1, NX):
                to_x = (x + k) % NX
                pltpu.make_async_remote_copy(
                    src_ref=xl.at[to_x // 2],
                    dst_ref=xlrecv.at[k - 1],
                    send_sem=xl_send,
                    recv_sem=xl_recv,
                    device_id=at(y, to_x, zh, tm),
                    device_id_type=MESH,
                ).start()

    for j in range(NY):
        to_y = (y + ORDER[j]) % NY
        pltpu.make_async_copy(xrecv.at[j], xrecv.at[j], x_recv.at[j]).wait()
        ysend[j] = (xbuf[x, to_y] + xrecv[j, 0]) + (xrecv[j, 1] + xrecv[j, 2])
        pltpu.make_async_remote_copy(
            src_ref=ysend.at[j, pl.ds(8, 8)],
            dst_ref=yrecv2.at[j],
            send_sem=y2_send,
            recv_sem=y2_recv,
            device_id=at(to_y, xp, zh, tm),
            device_id_type=MESH,
        ).start()
        if j < NY - 1:
            pltpu.make_async_remote_copy(
                src_ref=ysend.at[j],
                dst_ref=yrecv.at[j],
                send_sem=y_send,
                recv_sem=y_recv,
                device_id=at(to_y, x, zh, tm),
                device_id_type=MESH,
            ).start()
        if j == 0:
            pltpu.make_async_copy(xlrecv, xlrecv, xl_recv).wait()
            yl[...] = (xl[x // 2] + xlrecv[0]) + (xlrecv[1] + xlrecv[2])
            for i in range(NY - 1):
                line_y = (y + ORDER[i]) % NY
                pltpu.make_async_remote_copy(
                    src_ref=yl.at[line_y],
                    dst_ref=ylrecv.at[i],
                    send_sem=yl_send,
                    recv_sem=yl_recv,
                    device_id=at(line_y, x, zh, tm),
                    device_id_type=MESH,
                ).start()

    pltpu.make_async_copy(ylrecv, ylrecv, yl_recv).wait()
    total = yl[y]
    for i in range(NY - 1):
        total = total + ylrecv[i]
    zl[...] = total
    zlrecv[zh * NTM + tm] = total
    for kz in range(NZH):
        for kt in range(NTM):
            if kz or kt:
                pltpu.make_async_remote_copy(
                    src_ref=zl,
                    dst_ref=zlrecv.at[zh * NTM + tm],
                    send_sem=zl_send,
                    recv_sem=zl_recv,
                    device_id=at(y, x, (zh + kz) % NZH, (tm + kt) % NTM),
                    device_id_type=MESH,
                ).start()

    pltpu.make_async_copy(yrecv, yrecv, y_recv).wait()
    pltpu.make_async_copy(yrecv2, yrecv2, y2_recv).wait()
    own = ysend[NY - 1]
    for j in range(NY - 1):
        own = own + yrecv[j]
    other = yrecv2[0]
    for j in range(1, NY):
        other = other + yrecv2[j]
    diag, off = own[0:8], own[8:16]
    first = p == 0
    left, right = jnp.where(first, diag, off), jnp.where(first, off, diag)
    upper, lower = jnp.where(first, diag, other), jnp.where(first, other, diag)

    def turned(tile, shift):
        shift = shift % 128
        return pltpu.roll(tile, shift, 1) if shift else tile

    columns = [turned(t, -32 * ib) for t in (upper, lower) for ib in range(4)]
    columns = jnp.concatenate(columns + columns, axis=0)
    flipped = columns.T
    for ib in range(4):
        r0 = 8 * ib
        rows = jnp.where(lane < 32, turned(left, -32 * ib), turned(right, 32 - 32 * ib))
        rows = jnp.where(low, rows, flipped[r0 : r0 + 8])
        zsend[ib // 2, 8 * (ib % 2) : 8 * (ib % 2) + 8, :] = rows
    zrecv[zh * NTM + tm] = zsend[zh]
    for kz in range(NZH):
        for kt in range(NTM):
            if kz or kt:
                to_z = (zh + kz) % NZH
                pltpu.make_async_remote_copy(
                    src_ref=zsend.at[to_z],
                    dst_ref=zrecv.at[zh * NTM + tm],
                    send_sem=z_send,
                    recv_sem=z_recv,
                    device_id=at(y, x, to_z, (tm + kt) % NTM),
                    device_id_type=MESH,
                ).start()

    number = gid_ref[2 * y + x // 2]
    half = 0.5 * gram_scale
    re_t = pick(number, [half * (t[2] - t[3]) for t in TABLE])
    re_f = pick(number, [half * t[4] * (t[2] + t[3]) for t in TABLE])
    im_t = pick(number, [half * (t[2] + t[3]) for t in TABLE])
    im_f = pick(number, [half * t[4] * (t[3] - t[2]) for t in TABLE])
    phase_re = pick(number, [float(t[2]) for t in TABLE])
    phase_im = pick(number, [float(t[3]) for t in TABLE])
    straight = jnp.where(low1, re_t, im_f)
    crossed = jnp.where(low1, re_f, im_t)
    turn = jnp.where(low1, -phase_im, phase_im)

    pltpu.make_async_copy(zlrecv.at[pl.ds(0, 15)], zlrecv.at[pl.ds(0, 15)], zl_recv).wait()
    value = (zlrecv[0:NTM] + zlrecv[NTM : 2 * NTM]).reshape(NTM, 128)
    value = phase_re * value + turn * pltpu.roll(value, 64, 1)
    value = pltpu.roll(value, (128 - 16 * (2 * p + zh)) % 128, 1)
    loop_ref[:, 0, :] = value[:, 0:16]
    loop_ref[:, 1, :] = value[:, 64:80]

    pltpu.make_async_copy(zrecv.at[pl.ds(0, 15)], zrecv.at[pl.ds(0, 15)], z_recv).wait()
    for t in range(NTM):
        value = zrecv[t] + zrecv[NTM + t]
        gram_ref[t] = straight * value + crossed * pltpu.roll(value, 64, 1)

    pltpu.make_async_copy(xbuf.at[pl.ds(0, 3)], xbuf.at[pl.ds(0, 3)], x_send).wait()
    pltpu.make_async_copy(xlrecv, xlrecv, xl_send).wait()
    pltpu.make_async_copy(yrecv, yrecv, y_send).wait()
    pltpu.make_async_copy(yrecv2, yrecv2, y2_send).wait()
    pltpu.make_async_copy(ylrecv, ylrecv, yl_send).wait()
    pltpu.make_async_copy(zrecv.at[pl.ds(0, 15)], zrecv.at[pl.ds(0, 15)], z_send).wait()
    pltpu.make_async_copy(zlrecv.at[pl.ds(0, 15)], zlrecv.at[pl.ds(0, 15)], zl_send).wait()


def shards(vectors, dilution, gamma_ids):
    slices, count, halves, comps, sites = vectors.shape
    total_sites = sites * lax.axis_size("space")
    gram_scale = 1.0 / math.sqrt(48.0 * total_sites)
    loop_scale = 1.0 / math.sqrt(1.0 * total_sites)
    flat = vectors.transpose(0, 1, 3, 2, 4).reshape(count * comps * halves, sites)
    operands = (gamma_ids, dilution.reshape(1, count), flat)
    f32, bf16 = jnp.float32, jnp.bfloat16
    dma = pltpu.SemaphoreType.DMA
    vmem = pltpu.VMEM
    gram, loops = pl.pallas_call(
        partial(kernel, gram_scale, loop_scale),
        out_shape=(
            jax.ShapeDtypeStruct((NTM, 16, 128), f32),
            jax.ShapeDtypeStruct((NTM, 2, 16), f32),
        ),
        in_specs=[
            pl.BlockSpec(memory_space=pltpu.HBM),
            pl.BlockSpec(memory_space=pltpu.HBM),
            pl.BlockSpec(memory_space=pltpu.HBM),
        ],
        out_specs=(
            pl.BlockSpec(memory_space=pltpu.VMEM),
            pl.BlockSpec(memory_space=pltpu.VMEM),
        ),
        scratch_shapes=[
            pltpu.SMEM((NG,), jnp.int32),
            vmem((1, NV), jnp.int32),
            vmem((1536, 128), bf16),
            vmem((1536, 128), f32),
            vmem((528, 768), bf16),
            vmem((256, 256), f32),
            vmem((16, 2, 16, 128), f32),
            vmem((16, 1, 128), f32),
            vmem((NX, NY, 16, 128), f32),
            vmem((NY, NX - 1, 16, 128), f32),
            vmem((NY, 16, 128), f32),
            vmem((NY - 1, 16, 128), f32),
            vmem((NY, 8, 128), f32),
            vmem((NZH, 16, 128), f32),
            vmem((NZH * NTM, 16, 128), f32),
            vmem((2, NY, 1, 128), f32),
            vmem((NX - 1, NY, 1, 128), f32),
            vmem((NY, 1, 128), f32),
            vmem((NY - 1, 1, 128), f32),
            vmem((1, 128), f32),
            vmem((NZH * NTM, 1, 128), f32),
            dma,
            dma,
            dma,
            dma,
            dma((NY,)),
        ]
        + [dma] * 12,
        compiler_params=pltpu.CompilerParams(
            collective_id=0, has_side_effects=True, vmem_limit_bytes=8 << 20
        ),
        name="gram_loops",
    )(*[pltpu.with_memory_space_constraint(a, pltpu.HBM) for a in operands])
    return gram, loops.transpose(0, 2, 1)


def solution(mesh):
    placed = (P("tm", None, None, None, "space"), P(), P())
    return jax.shard_map(
        shards,
        mesh=mesh,
        in_specs=placed,
        out_specs=(P(None, "space", None), P(None, "space", None)),
        check_vma=False,
    )
```
